1024 devices in a mesh: seq: 128 (over y, z), tensor: 8 (over x, core).
Axes of the slice: x: 4, y: 8, z: 16, core: 2. Of those that a mesh axis runs over, the one named last changes fastest.
Arguments:
- queries: bfloat16 [12288, 4096], P('seq', 'tensor'), may hold values from -96 to 96
- keys: bfloat16 [12288, 1024], P('seq', 'tensor'), may hold values from -96 to 96
- values: bfloat16 [12288, 1024], P('seq', 'tensor'), may hold values from -6 to 6
- out_weight: bfloat16 [4096, 4096], P('tensor'), may hold values from -0.09375 to 0.09375
- doc_lengths: int32 [16], replicated, may hold values from 1 to 3072, 12288 in all
- stretch_place: int32 [256], replicated, may hold values from 0 to 255, each once
Outputs:
- output: bfloat16 [12288, 4096], P('seq', 'tensor')
The draws below stay inside these ranges and needn't reach their ends.
Inputs may be any that keep to these rules, and one draw needn't show every extreme that they name: `stretch_place`: each stored block number appears once. `doc_lengths`: the lengths sum to 12288; the longest is exactly 3072.
All inputs are finite; a program needn't handle non-finite values.
Results may differ from the reference program's by a relative error of at most 0.015.
Values may be sent and summed in bfloat16 or wider, within the bound.
No kernel may reach another device: no remote copies, remote signals or barrier semaphores. Data moves between devices by JAX's collectives and lax.ppermute only.
A program may use at most 64 MiB of HBM per device.

```python
import math
import jax
import jax.numpy as jnp
import numpy as np
from jax import lax

D = 4096
HEADS = 32
KV_HEADS = 8
HD = 128
TOK_DEV = 96
DOCS = 16
TOKENS = 12288
BLOCKS = 256
DOC_MOST = 3072


def draw_pair(key):
    base = jax.random.fold_in(key, 7)
    key_query, key_key = jax.random.split(base, 2)
    query_draw = jax.random.normal(key_query, (TOKENS, HEADS * HD), jnp.float32)
    key_draw = jax.random.normal(key_key, (TOKENS, KV_HEADS * HD), jnp.float32)
    query_draw = jnp.clip(query_draw, -96.0, 96.0)
    key_draw = jnp.clip(key_draw, -96.0, 96.0)
    return (query_draw, key_draw)


def draw_queries(key, part):
    return draw_pair(key)[0].astype(jnp.bfloat16)


def draw_keys(key, part):
    return draw_pair(key)[1].astype(jnp.bfloat16)


def levels(key, extent, cuts, low, largest):
    level = 1.0
    for position, shards_of in cuts:
        draws = jax.random.uniform(jax.random.fold_in(jax.random.fold_in(key, 6), position), (shards_of,), jnp.float32, low / len(cuts), largest / len(cuts))
        level = level * jnp.repeat(jnp.exp(draws), extent[position] // shards_of).reshape((-1,) + (1,) * (len(extent) - 1 - position))
    return level


def split_up(number_of, total, reach, skew):
    portions = [(1 << 20) // math.isqrt(rank ** skew) + 1 for rank in range(2, number_of + 1)]
    spare, holding = total - reach - (number_of - 1), [1] * (number_of - 1)
    while spare > 0:
        movable = [i for i in range(number_of - 1) if holding[i] < reach]
        whole, budget = sum([portions[i] for i in movable]), spare
        for i in movable:
            more = min(reach - holding[i], max(1, budget * portions[i] // whole), spare)
            holding[i] = holding[i] + more
            spare = spare - more
    return np.array([reach] + holding)


def ragged_sizes(rng, count, total, limit, slope):
    if count == 2:
        one = jax.random.randint(rng, (), max(1, total - limit), min(limit, total - 1) + 1)
        return jnp.stack([one, total - one])
    tallies = jnp.asarray(split_up(count, total, limit, slope), jnp.int32)
    twos = (count - 1) // 2
    donor, sink = tallies[1:1 + 2 * twos:2], tallies[2:2 + 2 * twos:2]
    room = jnp.minimum(donor - 1, limit - sink)
    moved = jax.random.randint(jax.random.fold_in(rng, 1), (twos,), 0, 1 << 20) % (room + 1)
    tallies = tallies.at[1:1 + 2 * twos:2].set(donor - moved).at[2:2 + 2 * twos:2].set(sink + moved)
    return tallies[jax.random.permutation(jax.random.fold_in(rng, 2), count)]


def normal_values(own_key, shape, scale, reach, cuts=(), kind=jnp.bfloat16):
    drawn = jax.random.normal(own_key, shape, jnp.float32) * scale
    if len(cuts) > 0:
        drawn = levels(own_key, shape, cuts, -0.22, 0.18) * drawn
    return jnp.clip(drawn, min=-reach, max=reach).astype(kind)


def setup_inputs(seed: int = 0) -> dict:
    key_list = jax.random.split(jax.random.key(seed), 7)
    return {
        "queries": draw_queries(jax.random.fold_in(key_list[6], 71), 0),
        "keys": draw_keys(jax.random.fold_in(key_list[6], 71), 0),
        "values": normal_values(key_list[2], (TOKENS, KV_HEADS * HD), 1.0, 6.0, ((0, 128), (1, 8))),
        "out_weight": normal_values(key_list[3], (HEADS * HD, D), (HEADS * HD) ** -0.5, 0.09375, ((0, 8),)),
        "doc_lengths": ragged_sizes(key_list[4], DOCS, TOKENS, DOC_MOST, 2).astype(jnp.int32),
        "stretch_place": jax.random.permutation(key_list[5], BLOCKS).astype(jnp.int32),
    }


rope_base = 500000.0

def seq_positions(first, count, stretch_place, block_rows):
    row_index = first + jnp.arange(count, dtype=jnp.int32)
    return (stretch_place[row_index // block_rows] * block_rows + row_index % block_rows).astype(jnp.int32)

def documents(positions, doc_lengths):
    ends = jnp.cumsum(doc_lengths).astype(jnp.int32)
    return lax.optimization_barrier(jnp.sum((ends[None, :] <= positions[:, None]).astype(jnp.int32), axis=1))

def rotary(heads_in, positions):
    width = heads_in.shape[-1]
    half = width // 2
    freqs = rope_base ** (-(2.0 / width) * jnp.arange(half, dtype=jnp.float32))
    angles = positions.astype(jnp.float32)[:, None] * freqs[None, :]
    cosine = jnp.cos(angles)[:, None, :]
    sine = jnp.sin(angles)[:, None, :]
    floats = heads_in.astype(jnp.float32)
    first_half = floats[..., :half]
    second_half = floats[..., half:]
    rotated = jnp.concatenate([first_half * cosine - second_half * sine, second_half * cosine + first_half * sine], axis=-1)
    return rotated.astype(jnp.bfloat16)

def reference(queries, keys, values, out_weight, doc_lengths, stretch_place):
    block_rows = TOK_DEV // 2
    positions = seq_positions(0, TOKENS, stretch_place, block_rows)
    document = documents(positions, doc_lengths)
    q_rot = rotary(queries.reshape(TOKENS, HEADS, HD), positions)
    k_rot = rotary(keys.reshape(TOKENS, KV_HEADS, HD), positions)
    value_heads = values.reshape(TOKENS, KV_HEADS, HD)
    order = jnp.zeros((TOKENS,), jnp.int32).at[positions].set(jnp.arange(TOKENS, dtype=jnp.int32))
    q_sorted = q_rot[order]
    k_padded = jnp.concatenate([jnp.zeros((DOC_MOST, KV_HEADS, HD), jnp.bfloat16), k_rot[order]], axis=0)
    v_padded = jnp.concatenate([jnp.zeros((DOC_MOST, KV_HEADS, HD), jnp.bfloat16), value_heads[order]], axis=0)
    doc_sorted = document[order].astype(jnp.int32)
    doc_padded = jnp.concatenate([jnp.full((DOC_MOST,), -1, jnp.int32), doc_sorted], axis=0)
    group = HEADS // KV_HEADS
    scale = 1.0 / math.sqrt(HD)
    window = DOC_MOST + block_rows

    def one_block(index):
        start = (index * block_rows).astype(jnp.int32)
        q_block = lax.dynamic_slice_in_dim(q_sorted, start, block_rows, 0)
        k_block = lax.dynamic_slice_in_dim(k_padded, start, window, 0)
        v_block = lax.dynamic_slice_in_dim(v_padded, start, window, 0)
        q_docs = lax.dynamic_slice_in_dim(doc_sorted, start, block_rows, 0)
        k_docs = lax.dynamic_slice_in_dim(doc_padded, start, window, 0)
        q_pos = start + jnp.arange(block_rows, dtype=jnp.int32)
        k_pos = start - DOC_MOST + jnp.arange(window, dtype=jnp.int32)
        allowed = (k_pos[None, :] <= q_pos[:, None]) & (k_docs[None, :] == q_docs[:, None]) & (k_pos[None, :] >= 0)
        q_float = q_block.astype(jnp.float32).reshape(block_rows, KV_HEADS, group, HD)
        scores = jnp.einsum('tkgd,nkd->kgtn', q_float, k_block.astype(jnp.float32)) * scale
        scores = jnp.where(allowed[None, None], scores, -1e+30)
        row_max = lax.optimization_barrier(jnp.max(scores, axis=-1, keepdims=True))
        weights = jnp.where(allowed[None, None], jnp.exp(scores - row_max), 0.0)
        totals = lax.optimization_barrier(jnp.sum(weights, axis=-1))
        rounded = weights.astype(jnp.bfloat16).astype(jnp.float32)
        mixed = jnp.einsum('kgtn,nkd->tkgd', rounded, v_block.astype(jnp.float32))
        mixed = mixed / jnp.transpose(totals, (2, 0, 1))[..., None]
        return mixed.reshape(block_rows, HEADS * HD)
    sorted_out = lax.map(one_block, jnp.arange(TOKENS // block_rows, dtype=jnp.int32))
    sorted_out = sorted_out.reshape(TOKENS, HEADS * HD)
    attended = sorted_out[positions].astype(jnp.bfloat16)
    return jnp.dot(attended, out_weight, preferred_element_type=jnp.float32).astype(jnp.bfloat16)
```

```python
import math

import jax
import jax.numpy as jnp
import numpy as np
from jax import lax
from jax.experimental import pallas as pl
from jax.experimental.pallas import tpu as pltpu
from jax.sharding import Mesh
from jax.sharding import PartitionSpec as P

HD = 128
HALF = HD // 2
BLOCK = 48
ROPE_BASE = 500000.0
NEG = -1e30
STAT = 16
SCALE = math.log2(math.e) / math.sqrt(HD)


def rope_tables(blocks):
    freqs = ROPE_BASE ** (-(2.0 / HD) * np.arange(HALF, dtype=np.float64))
    freqs = np.concatenate([freqs, freqs])
    start = (BLOCK * np.arange(blocks, dtype=np.float64))[:, None] * freqs
    row = np.arange(BLOCK, dtype=np.float64)[:, None] * freqs
    f32 = np.float32
    return (np.cos(start).astype(f32), np.sin(start).astype(f32), np.cos(row).astype(f32), np.sin(row).astype(f32))


def rotate_kernel(place, q, k, v, cos_start, sin_start, cos_row, sin_row, q_out, kv_out):
    heads = q.shape[1] // HD
    first = lax.axis_index("y") * lax.axis_size("z") + lax.axis_index("z")
    lane = lax.broadcasted_iota(jnp.int32, (BLOCK, HD), 1)
    for b in range(2):
        at = place[first * 2 + b]
        c0 = cos_start[pl.ds(at, 1), :]
        s0 = sin_start[pl.ds(at, 1), :]
        cosine = c0 * cos_row[...] - s0 * sin_row[...]
        sine = s0 * cos_row[...] + c0 * sin_row[...]
        sine = jnp.where(lane < HALF, -sine, sine)
        rows = pl.ds(b * BLOCK, BLOCK)
        for h in range(heads):
            x = q[rows, pl.ds(h * HD, HD)].astype(jnp.float32)
            y = x * cosine + pltpu.roll(x, HALF, 1) * sine
            q_out[rows, pl.ds(h * HD, HD)] = y.astype(jnp.bfloat16)
        x = k[rows, :].astype(jnp.float32)
        y = x * cosine + pltpu.roll(x, HALF, 1) * sine
        kv_out[rows, pl.ds(0, HD)] = y.astype(jnp.bfloat16)
        kv_out[rows, pl.ds(HD, HD)] = v[rows, :]


def attend_kernel(place, ends, q, kv, out, scores, values_t):
    heads = q.shape[2] // HD
    lanes = 2 * heads * BLOCK
    n_keys = kv.shape[0]
    n_blocks = n_keys // BLOCK
    z_size = lax.axis_size("z")
    my_y = lax.axis_index("y")
    my_z = lax.axis_index("z")
    peer = pl.program_id(0)

    @pl.when(peer == 0)
    def prepare():
        values_t[pl.ds(0, HD), :] = kv[:, pl.ds(HD, HD)].T
        values_t[pl.ds(HD, STAT), :] = jnp.ones((STAT, n_keys), jnp.bfloat16)

    base = (peer * z_size + my_z) * 2
    p0 = place[base] * BLOCK
    p1 = place[base + 1] * BLOCK
    lane = lax.broadcasted_iota(jnp.int32, (8, lanes), 1)
    q_pos = jnp.where(lane < heads * BLOCK, p0, p1) + lane % BLOCK
    q_start = jnp.zeros((8, lanes), jnp.int32)
    end = jnp.int32(0)
    for d in range(ends.shape[0]):
        end = end + ends[d]
        q_start = jnp.where(end <= q_pos, end, q_start)
    parts = []
    for b in range(2):
        for h in range(heads):
            parts.append(q[0, pl.ds(b * BLOCK, BLOCK), pl.ds(h * HD, HD)])
    q_rows = jnp.concatenate(parts, axis=0)
    sub = lax.broadcasted_iota(jnp.int32, (8, lanes), 0)
    top = jnp.full((8, lanes), NEG, jnp.float32)
    for j in range(n_blocks):
        s = lax.dot_general(
            kv[pl.ds(j * BLOCK, BLOCK), pl.ds(0, HD)],
            q_rows,
            (((1,), (1,)), ((), ())),
            preferred_element_type=jnp.float32,
        )
        k0 = place[my_y * n_blocks + j] * BLOCK
        for r in range(0, BLOCK, 8):
            k_pos = sub + (k0 + r)
            piece = jnp.where((k_pos <= q_pos) & (k_pos >= q_start), s[r : r + 8], NEG)
            scores[pl.ds(j * BLOCK + r, 8), :] = piece
            top = jnp.maximum(top, piece)
    top = jnp.max(top, axis=0, keepdims=True)
    safe = jnp.maximum(top, -1e29)
    weights = jnp.exp2((scores[...] - safe) * SCALE).astype(jnp.bfloat16)
    sums = jnp.dot(values_t[...], weights, preferred_element_type=jnp.float32)
    out[0, pl.ds(0, HD), :] = sums[:HD].astype(jnp.bfloat16)
    total = sums[HD : HD + 1]
    t0 = total.astype(jnp.bfloat16)
    t1 = (total - t0.astype(jnp.float32)).astype(jnp.bfloat16)
    m0 = top.astype(jnp.bfloat16)
    rest = top - m0.astype(jnp.float32)
    m1 = rest.astype(jnp.bfloat16)
    m2 = (rest - m1.astype(jnp.float32)).astype(jnp.bfloat16)
    zero = jnp.zeros((STAT - 5, lanes), jnp.bfloat16)
    out[0, pl.ds(HD, STAT), :] = jnp.concatenate([m0, m1, m2, t0, t1, zero], axis=0)


def project_kernel(parts, weight, out, rows):
    heads = rows.shape[1] // HD
    peers = parts.shape[0]

    @pl.when(pl.program_id(0) == 0)
    def combine():
        tops, totals = [], []
        for p in range(peers):
            stat = parts[p, pl.ds(HD, STAT), :].astype(jnp.float32)
            tops.append(stat[0:1] + stat[1:2] + stat[2:3])
            totals.append(stat[3:4] + stat[4:5])
        top = tops[0]
        for p in range(1, peers):
            top = jnp.maximum(top, tops[p])
        total = jnp.zeros_like(top)
        factors = []
        for p in range(peers):
            factor = jnp.exp2((tops[p] - top) * SCALE)
            total = total + factor * totals[p]
            factors.append(factor)
        total = 1.0 / total
        mixed = jnp.zeros((HD, top.shape[1]), jnp.float32)
        for p in range(peers):
            mixed = mixed + parts[p, pl.ds(0, HD), :].astype(jnp.float32) * (factors[p] * total)
        turned = mixed.T.astype(jnp.bfloat16)
        for b in range(2):
            for h in range(heads):
                at = (b * heads + h) * BLOCK
                rows[pl.ds(b * BLOCK, BLOCK), pl.ds(h * HD, HD)] = turned[at : at + BLOCK]

    out[0] = jnp.dot(rows[...], weight[...], preferred_element_type=jnp.float32).astype(jnp.bfloat16)


SMEM = pl.BlockSpec(memory_space=pltpu.SMEM)


def body(queries, keys, values, out_weight, doc_lengths, stretch_place):
    tok, q_width = queries.shape
    heads = q_width // HD
    ny, nz, nt = lax.axis_size("y"), lax.axis_size("z"), lax.axis_size("tensor")
    lanes = 2 * heads * BLOCK
    bf16 = jnp.bfloat16
    tables = [jnp.asarray(t) for t in rope_tables(stretch_place.shape[0])]
    vmem = pl.BlockSpec(memory_space=pltpu.VMEM)
    q_rot, kv = pl.pallas_call(
        rotate_kernel,
        out_shape=(jax.ShapeDtypeStruct((tok, q_width), bf16), jax.ShapeDtypeStruct((tok, 2 * HD), bf16)),
        in_specs=[SMEM] + [vmem] * 7,
        out_specs=(vmem, vmem),
        compiler_params=pltpu.CompilerParams(vmem_limit_bytes=8 << 20),
        name="rotate",
    )(stretch_place, queries, keys, values, *tables)
    kv_all = lax.all_gather(kv, "z", axis=0, tiled=True)
    q_all = gather_queries(q_rot, ny)
    n_keys = nz * tok
    parts = pl.pallas_call(
        attend_kernel,
        out_shape=jax.ShapeDtypeStruct((ny, HD + STAT, lanes), bf16),
        grid=(ny,),
        in_specs=[
            SMEM,
            SMEM,
            pl.BlockSpec((1, tok, q_width), lambda i: (i, 0, 0)),
            pl.BlockSpec((n_keys, 2 * HD), lambda i: (0, 0)),
        ],
        out_specs=pl.BlockSpec((1, HD + STAT, lanes), lambda i: (i, 0, 0)),
        scratch_shapes=[pltpu.VMEM((n_keys, lanes), jnp.float32), pltpu.VMEM((HD + STAT, n_keys), bf16)],
        compiler_params=pltpu.CompilerParams(vmem_limit_bytes=20 << 20),
        name="attend",
    )(stretch_place, doc_lengths, q_all, kv_all)
    parts = lax.all_to_all(parts, "y", split_axis=0, concat_axis=0, tiled=True)
    model = out_weight.shape[1]
    step = model // nt
    partial_rows = pl.pallas_call(
        project_kernel,
        out_shape=jax.ShapeDtypeStruct((nt, tok, step), bf16),
        grid=(nt,),
        in_specs=[
            pl.BlockSpec((ny, HD + STAT, lanes), lambda i: (0, 0, 0)),
            pl.BlockSpec((q_width, step), lambda i: (0, i)),
        ],
        out_specs=pl.BlockSpec((1, tok, step), lambda i: (i, 0, 0)),
        scratch_shapes=[pltpu.VMEM((tok, q_width), bf16)],
        compiler_params=pltpu.CompilerParams(vmem_limit_bytes=12 << 20),
        name="project",
    )(parts, out_weight)
    arrived = lax.all_to_all(partial_rows, "tensor", split_axis=0, concat_axis=0, tiled=True)
    return arrived.astype(jnp.float32).sum(axis=0).astype(bf16)


def gather_queries(q_rot, peers):
    same = jnp.broadcast_to(q_rot[None], (peers,) + q_rot.shape)
    return lax.all_to_all(same, "y", split_axis=0, concat_axis=0, tiled=True)


def solution(mesh, ny=8):
    n_seq, n_tensor = mesh.devices.shape
    inner = Mesh(mesh.devices.reshape(ny, n_seq // ny, n_tensor), ("y", "z", "tensor"))
    seq = ("y", "z")
    in_specs = (P(seq, "tensor"), P(seq, "tensor"), P(seq, "tensor"), P("tensor", None), P(), P())
    return jax.shard_map(body, mesh=inner, in_specs=in_specs, out_specs=P(seq, "tensor"), check_vma=False)
```

```python
import math

import jax
import jax.numpy as jnp
import numpy as np
from jax import lax
from jax.experimental import pallas as pl
from jax.experimental.pallas import tpu as pltpu
from jax.sharding import Mesh
from jax.sharding import PartitionSpec as P

HD = 128
HALF = HD // 2
BLOCK = 48
ROPE_BASE = 500000.0
BIG = 2.0**100
FLOOR = -1e29
FAR = 1 << 30
STAT = 16
CHUNK = 512
SCALE = math.log2(math.e) / math.sqrt(HD)
BF16 = jnp.bfloat16
F32 = jnp.float32


def rope_tables(blocks):
    freqs = ROPE_BASE ** (-(2.0 / HD) * np.arange(HALF, dtype=np.float64))
    freqs = np.concatenate([freqs, freqs])
    start = (BLOCK * np.arange(blocks, dtype=np.float64))[:, None] * freqs
    row = np.arange(BLOCK, dtype=np.float64)[:, None] * freqs
    return np.concatenate([np.cos(row), np.sin(row), np.cos(start), np.sin(start)]).astype(np.float32)


def rotate_kernel(place_in, q_in, k_in, v_in, table_in, q_out, kv_out, place, q, k, v, table, sems):
    sources = (place_in, table_in, q_in, k_in, v_in)
    copies = [pltpu.make_async_copy(s, d, sems.at[i]) for i, (s, d) in enumerate(zip(sources, (place, table, q, k, v)))]
    for copy in copies:
        copy.start()
    for copy in copies:
        copy.wait()
    heads = q.shape[1] // HD
    blocks = place.shape[0]
    first = lax.axis_index("y") * lax.axis_size("z") + lax.axis_index("z")
    lane = lax.broadcasted_iota(jnp.int32, (BLOCK, HD), 1)
    cos_row = table[pl.ds(0, BLOCK), :]
    sin_row = table[pl.ds(BLOCK, BLOCK), :]
    for b in range(2):
        at = place[first * 2 + b]
        c0 = table[pl.ds(2 * BLOCK + at, 1), :]
        s0 = table[pl.ds(2 * BLOCK + blocks + at, 1), :]
        cosine = c0 * cos_row - s0 * sin_row
        sine = s0 * cos_row + c0 * sin_row
        sine = jnp.where(lane < HALF, -sine, sine)
        rows = pl.ds(b * BLOCK, BLOCK)
        for h in range(heads):
            x = q[rows, pl.ds(h * HD, HD)].astype(F32)
            y = (x * cosine + pltpu.roll(x, HALF, 1) * sine).astype(BF16)
            for p in range(q_out.shape[0]):
                q_out[p, rows, pl.ds(h * HD, HD)] = y
        x = k[rows, :].astype(F32)
        y = x * cosine + pltpu.roll(x, HALF, 1) * sine
        kv_out[rows, pl.ds(0, HD)] = y.astype(BF16)
        kv_out[rows, pl.ds(HD, HD)] = v[rows, :]


def attend_kernel(place_in, docs_in, q, kv, out, place, docs, scores, values_t, keys, queries, sems):
    copies = [
        pltpu.make_async_copy(place_in, place, sems.at[0]),
        pltpu.make_async_copy(docs_in, docs, sems.at[1]),
    ]
    for copy in copies:
        copy.start()
    peers, tok, width = q.shape
    heads = width // HD
    lanes = 2 * heads * BLOCK
    n_keys = kv.shape[0]
    n_blocks = n_keys // BLOCK
    n_docs = docs.shape[0]
    z_size = lax.axis_size("z")
    my_y = lax.axis_index("y")
    my_z = lax.axis_index("z")
    values_t[pl.ds(0, HD), :] = kv[:, pl.ds(HD, HD)].T
    values_t[pl.ds(HD, STAT), :] = jnp.ones((STAT, n_keys), BF16)
    keys[:, pl.ds(0, HD)] = kv[:, pl.ds(0, HD)]
    for copy in copies:
        copy.wait()

    lane = lax.broadcasted_iota(jnp.int32, (1, HD), 1)
    begin = jnp.full((1, HD), FAR, jnp.int32)
    end = jnp.full((1, HD), FAR, jnp.int32)
    edge = jnp.int32(0)
    for d in range(n_docs):
        begin = jnp.where(lane == d, edge, begin)
        edge = edge + docs[d]
        end = jnp.where(lane == d, edge, end)
    causal_at = n_docs
    own_at = causal_at + 2 * peers
    assert own_at + 2 * BLOCK <= HD
    for p in range(peers):
        for b in range(2):
            after = (place[(p * z_size + my_z) * 2 + b] + 1) * BLOCK
            begin = jnp.where(lane == causal_at + 2 * p + b, after, begin)
    for b in range(2):
        at = own_at + b * BLOCK
        mine = (lane >= at) & (lane < at + BLOCK)
        key_at = place[(my_y * z_size + my_z) * 2 + b] * BLOCK + lane - at
        begin = jnp.where(mine, key_at, begin)
        end = jnp.where(mine, key_at + 1, end)

    row = lax.broadcasted_iota(jnp.int32, (BLOCK, HD), 0)
    wide = lax.broadcasted_iota(jnp.int32, (BLOCK, HD), 1)

    def key_columns(j, _):
        k_pos = row + place[my_y * n_blocks + j] * BLOCK
        inside = (k_pos >= begin) & (k_pos < end)
        at = pl.multiple_of(j * BLOCK, BLOCK)
        keys[pl.ds(at, BLOCK), pl.ds(HD, HD)] = jnp.where(inside, -BIG, 0.0).astype(BF16)
        return 0

    lax.fori_loop(0, n_blocks, key_columns, 0, unroll=4)

    def one_peer(p, _):
        for b in range(2):
            q_pos = row + place[(p * z_size + my_z) * 2 + b] * BLOCK
            doc = jnp.where((q_pos < begin) | (q_pos >= end), 1.0, 0.0)
            block = jnp.where((q_pos >= begin - BLOCK) & (q_pos < begin), 1.0, 0.0)
            later = jnp.where(q_pos < begin, 1.0, 0.0)
            columns = jnp.where(wide < causal_at, doc, jnp.where(wide < own_at, block, later)).astype(BF16)
            for h in range(heads):
                rows = pl.ds((b * heads + h) * BLOCK, BLOCK)
                queries[rows, pl.ds(0, HD)] = q[p, pl.ds(b * BLOCK, BLOCK), pl.ds(h * HD, HD)]
                queries[rows, pl.ds(HD, HD)] = columns
        top = jnp.full((8, lanes), -4.0 * BIG, F32)
        for at in range(0, n_keys, CHUNK):
            size = min(CHUNK, n_keys - at)
            s = lax.dot_general(
                keys[pl.ds(at, size), :],
                queries[...],
                (((1,), (1,)), ((), ())),
                preferred_element_type=F32,
            )
            scores[pl.ds(at, size), :] = s
            top = jnp.maximum(top, jnp.max(s.reshape(size // 8, 8, lanes), axis=0))
        top = jnp.max(top, axis=0, keepdims=True)
        safe = jnp.maximum(top, FLOOR)
        sums = jnp.zeros((HD + STAT, lanes), F32)
        for at in range(0, n_keys, CHUNK):
            size = min(CHUNK, n_keys - at)
            weights = jnp.exp2((scores[pl.ds(at, size), :] - safe) * SCALE).astype(BF16)
            sums = sums + jnp.dot(values_t[:, pl.ds(at, size)], weights, preferred_element_type=F32)
        out[p, pl.ds(0, HD), :] = sums[:HD].astype(BF16)
        total = sums[HD : HD + 1]
        t0 = total.astype(BF16)
        t1 = (total - t0.astype(F32)).astype(BF16)
        m0 = top.astype(BF16)
        rest = top - m0.astype(F32)
        m1 = rest.astype(BF16)
        m2 = (rest - m1.astype(F32)).astype(BF16)
        zero = jnp.zeros((STAT - 5, lanes), BF16)
        out[p, pl.ds(HD, STAT), :] = jnp.concatenate([m0, m1, m2, t0, t1, zero], axis=0)
        return 0

    lax.fori_loop(0, peers, one_peer, 0)


def combine_kernel(parts, weight, rows, given):
    heads = rows.shape[1] // HD
    peers = parts.shape[0]
    tops, totals = [], []
    for p in range(peers):
        stat = parts[p, pl.ds(HD, STAT), :].astype(F32)
        tops.append(stat[0:1] + stat[1:2] + stat[2:3])
        totals.append(stat[3:4] + stat[4:5])
    top = tops[0]
    for p in range(1, peers):
        top = jnp.maximum(top, tops[p])
    total = jnp.zeros_like(top)
    factors = []
    for p in range(peers):
        factor = jnp.exp2((tops[p] - top) * SCALE)
        total = total + factor * totals[p]
        factors.append(factor)
    total = 1.0 / total
    factors = [f * total for f in factors]
    mixed = parts[0, pl.ds(0, HD), :].astype(F32) * factors[0]
    for p in range(1, peers):
        mixed = mixed + parts[p, pl.ds(0, HD), :].astype(F32) * factors[p]
    turned = mixed.T.astype(BF16)
    for b in range(2):
        for h in range(heads):
            at = (b * heads + h) * BLOCK
            rows[pl.ds(b * BLOCK, BLOCK), pl.ds(h * HD, HD)] = turned[at : at + BLOCK]
    project(rows, weight, given, 1 - lax.axis_index("c"))


def keep_kernel(rows, weight, kept):
    project(rows, weight, kept, lax.axis_index("c"))


def project(rows, weight, out, core):
    step = out.shape[2]
    for x in range(out.shape[0]):
        columns = pl.ds(pl.multiple_of((2 * x + core) * step, step), step)
        out[x] = jnp.dot(rows[...], weight[:, columns], preferred_element_type=F32).astype(out.dtype)


def body(queries, keys, values, out_weight, doc_lengths, stretch_place):
    tok, q_width = queries.shape
    heads = q_width // HD
    ny, nz, nx = lax.axis_size("y"), lax.axis_size("z"), lax.axis_size("x")
    lanes = 2 * heads * BLOCK
    table = rope_tables(stretch_place.shape[0])
    vmem = pl.BlockSpec(memory_space=pltpu.VMEM)
    hbm = pl.BlockSpec(memory_space=pltpu.HBM)
    n_place = stretch_place.shape[0]
    n_docs = doc_lengths.shape[0]
    q_rot, kv = pl.pallas_call(
        rotate_kernel,
        out_shape=(jax.ShapeDtypeStruct((ny, tok, q_width), BF16), jax.ShapeDtypeStruct((tok, 2 * HD), BF16)),
        in_specs=[hbm] * 5,
        out_specs=(vmem, vmem),
        scratch_shapes=[
            pltpu.SMEM((n_place,), jnp.int32),
            pltpu.VMEM((tok, q_width), BF16),
            pltpu.VMEM((tok, HD), BF16),
            pltpu.VMEM((tok, HD), BF16),
            pltpu.VMEM(table.shape, F32),
            pltpu.SemaphoreType.DMA((5,)),
        ],
        compiler_params=pltpu.CompilerParams(vmem_limit_bytes=4 << 20),
        name="rotate",
    )(*[pltpu.with_memory_space_constraint(a, pltpu.HBM) for a in (stretch_place, queries, keys, values, jnp.asarray(table))])
    q_all = lax.all_to_all(q_rot, "y", split_axis=0, concat_axis=0, tiled=True)
    kv_all = lax.all_gather(kv, "z", axis=0, tiled=True)
    n_keys = nz * tok
    pairs = ny * lanes * n_keys
    parts = pl.pallas_call(
        attend_kernel,
        out_shape=jax.ShapeDtypeStruct((ny, HD + STAT, lanes), BF16),
        in_specs=[hbm, hbm, vmem, vmem],
        out_specs=vmem,
        scratch_shapes=[
            pltpu.SMEM((n_place,), jnp.int32),
            pltpu.SMEM((n_docs,), jnp.int32),
            pltpu.VMEM((n_keys, lanes), F32),
            pltpu.VMEM((HD + STAT, n_keys), BF16),
            pltpu.VMEM((n_keys, 2 * HD), BF16),
            pltpu.VMEM((lanes, 2 * HD), BF16),
            pltpu.SemaphoreType.DMA((2,)),
        ],
        compiler_params=pltpu.CompilerParams(vmem_limit_bytes=16 << 20),
        cost_estimate=pl.CostEstimate(flops=4 * pairs * HD, bytes_accessed=4 << 20, transcendentals=pairs),
        name="attend",
    )(
        pltpu.with_memory_space_constraint(stretch_place, pltpu.HBM),
        pltpu.with_memory_space_constraint(doc_lengths, pltpu.HBM),
        q_all,
        kv_all,
    )
    parts = lax.all_to_all(parts, "y", split_axis=0, concat_axis=0, tiled=True)
    step = out_weight.shape[1] // (2 * nx)
    half_flops = 2 * tok * q_width * nx * step
    cost = pl.CostEstimate(flops=half_flops, bytes_accessed=4 << 20, transcendentals=0)
    rows, given = pl.pallas_call(
        combine_kernel,
        out_shape=(jax.ShapeDtypeStruct((tok, q_width), BF16), jax.ShapeDtypeStruct((nx, tok, step), BF16)),
        in_specs=[vmem, vmem],
        out_specs=(vmem, vmem),
        compiler_params=pltpu.CompilerParams(vmem_limit_bytes=8 << 20),
        cost_estimate=cost,
        name="combine",
    )(parts, out_weight)
    got = lax.ppermute(given, "c", [(0, 1), (1, 0)])
    kept = pl.pallas_call(
        keep_kernel,
        out_shape=jax.ShapeDtypeStruct((nx, tok, step), F32),
        in_specs=[vmem, vmem],
        out_specs=vmem,
        compiler_params=pltpu.CompilerParams(vmem_limit_bytes=8 << 20),
        cost_estimate=cost,
        name="keep",
    )(rows, out_weight)
    both = (kept + got.astype(F32)).astype(BF16)
    arrived = lax.all_to_all(both, "x", split_axis=0, concat_axis=0, tiled=True)
    return arrived.astype(F32).sum(axis=0).astype(BF16)


def solution(mesh, ny=8):
    n_seq, n_tensor = mesh.devices.shape
    shape = (ny, n_seq // ny, n_tensor // 2, 2)
    inner = Mesh(mesh.devices.reshape(shape), ("y", "z", "x", "c"))
    seq, tensor = ("y", "z"), ("x", "c")
    split = P(seq, tensor)
    in_specs = (split, split, split, P(tensor, None), P(), P())
    return jax.shard_map(body, mesh=inner, in_specs=in_specs, out_specs=split, check_vma=False)
```

```python
import math

import jax
import jax.numpy as jnp
import numpy as np
from jax import lax
from jax.experimental import pallas as pl
from jax.experimental.pallas import tpu as pltpu
from jax.sharding import Mesh
from jax.sharding import PartitionSpec as P

HD = 128
HALF = HD // 2
BLOCK = 48
ROPE_BASE = 500000.0
BIG = 2.0**100
FLOOR = -1e29
FAR = 1 << 30
STAT = 8
CHUNK = 256
PEERS = 2
SCALE = math.log2(math.e) / math.sqrt(HD)
BF16 = jnp.bfloat16
F32 = jnp.float32


def rope_tables(blocks):
    freqs = ROPE_BASE ** (-(2.0 / HD) * np.arange(HALF, dtype=np.float64))
    freqs = np.concatenate([freqs, freqs])
    start = (BLOCK * np.arange(blocks, dtype=np.float64))[:, None] * freqs
    row = np.arange(BLOCK, dtype=np.float64)[:, None] * freqs
    return np.concatenate([np.cos(row), np.sin(row), np.cos(start), np.sin(start)]).astype(np.float32)


def rotate_kernel(place_in, q_in, k_in, v_in, table_in, q_out, kv_out, place, q, k, v, table, sems):
    sources = (place_in, table_in, q_in, k_in, v_in)
    copies = [pltpu.make_async_copy(s, d, sems.at[i]) for i, (s, d) in enumerate(zip(sources, (place, table, q, k, v)))]
    for copy in copies:
        copy.start()
    for copy in copies:
        copy.wait()
    heads = q.shape[1] // HD
    blocks = place.shape[0]
    first = lax.axis_index("y") * lax.axis_size("z") + lax.axis_index("z")
    lane = lax.broadcasted_iota(jnp.int32, (BLOCK, HD), 1)
    cos_row = table[pl.ds(0, BLOCK), :]
    sin_row = table[pl.ds(BLOCK, BLOCK), :]
    for b in range(2):
        at = place[first * 2 + b]
        c0 = table[pl.ds(2 * BLOCK + at, 1), :]
        s0 = table[pl.ds(2 * BLOCK + blocks + at, 1), :]
        cosine = c0 * cos_row - s0 * sin_row
        sine = s0 * cos_row + c0 * sin_row
        sine = jnp.where(lane < HALF, -sine, sine)
        rows = pl.ds(b * BLOCK, BLOCK)
        for h in range(heads):
            x = q[rows, pl.ds(h * HD, HD)].astype(F32)
            y = (x * cosine + pltpu.roll(x, HALF, 1) * sine).astype(BF16)
            for p in range(q_out.shape[0]):
                q_out[p, rows, pl.ds(h * HD, HD)] = y
        x = k[rows, :].astype(F32)
        y = x * cosine + pltpu.roll(x, HALF, 1) * sine
        kv_out[rows, pl.ds(0, HD)] = y.astype(BF16)
        kv_out[rows, pl.ds(HD, HD)] = v[rows, :]


def attend_kernel(place_in, docs_in, q, kv, out, place, docs, scores, weights, values_t, keys, queries, sems):
    copies = [
        pltpu.make_async_copy(place_in, place, sems.at[0]),
        pltpu.make_async_copy(docs_in, docs, sems.at[1]),
    ]
    for copy in copies:
        copy.start()
    peers, tok, width = q.shape
    heads = width // HD
    lanes = 2 * heads * BLOCK
    n_keys = kv.shape[0]
    n_blocks = n_keys // BLOCK
    n_docs = docs.shape[0]
    z_size = lax.axis_size("z")
    my_y = lax.axis_index("y")
    my_z = lax.axis_index("z")
    values_t[pl.ds(0, HD), :] = kv[:, pl.ds(HD, HD)].T
    values_t[pl.ds(HD, STAT), :] = jnp.ones((STAT, n_keys), BF16)
    keys[:, pl.ds(0, HD)] = kv[:, pl.ds(0, HD)]
    for copy in copies:
        copy.wait()

    lane = lax.broadcasted_iota(jnp.int32, (1, HD), 1)
    begin = jnp.full((1, HD), FAR, jnp.int32)
    end = jnp.full((1, HD), FAR, jnp.int32)
    edge = jnp.int32(0)
    for d in range(n_docs):
        begin = jnp.where(lane == d, edge, begin)
        edge = edge + docs[d]
        end = jnp.where(lane == d, edge, end)
    causal_at = n_docs
    own_at = causal_at + 2 * peers
    assert own_at + 2 * BLOCK <= HD
    for p in range(peers):
        for b in range(2):
            after = (place[(p * z_size + my_z) * 2 + b] + 1) * BLOCK
            begin = jnp.where(lane == causal_at + 2 * p + b, after, begin)
    for b in range(2):
        at = own_at + b * BLOCK
        mine = (lane >= at) & (lane < at + BLOCK)
        key_at = place[(my_y * z_size + my_z) * 2 + b] * BLOCK + lane - at
        begin = jnp.where(mine, key_at, begin)
        end = jnp.where(mine, key_at + 1, end)

    row = lax.broadcasted_iota(jnp.int32, (BLOCK, HD), 0)
    wide = lax.broadcasted_iota(jnp.int32, (BLOCK, HD), 1)

    def key_columns(j, _):
        k_pos = row + place[my_y * n_blocks + j] * BLOCK
        inside = (k_pos >= begin) & (k_pos < end)
        at = pl.multiple_of(j * BLOCK, BLOCK)
        keys[pl.ds(at, BLOCK), pl.ds(HD, HD)] = jnp.where(inside, -BIG, 0.0).astype(BF16)
        return 0

    lax.fori_loop(0, n_blocks, key_columns, 0, unroll=4)

    groups = peers // PEERS
    wide_lanes = PEERS * lanes
    starts = list(range(0, n_keys, CHUNK))

    def set_queries(g):
        for i in range(PEERS):
            p = g * PEERS + i
            for b in range(2):
                q_pos = row + place[(p * z_size + my_z) * 2 + b] * BLOCK
                doc = jnp.where((q_pos < begin) | (q_pos >= end), 1.0, 0.0)
                block = jnp.where((q_pos >= begin - BLOCK) & (q_pos < begin), 1.0, 0.0)
                later = jnp.where(q_pos < begin, 1.0, 0.0)
                columns = jnp.where(wide < causal_at, doc, jnp.where(wide < own_at, block, later)).astype(BF16)
                for h in range(heads):
                    rows = pl.ds(((i * 2 + b) * heads + h) * BLOCK, BLOCK)
                    queries[g % 2, rows, pl.ds(0, HD)] = q[p, pl.ds(b * BLOCK, BLOCK), pl.ds(h * HD, HD)]
                    queries[g % 2, rows, pl.ds(HD, HD)] = columns

    def score(g, at, top):
        size = min(CHUNK, n_keys - at)
        s = lax.dot_general(
            keys[pl.ds(at, size), :],
            queries[g % 2],
            (((1,), (1,)), ((), ())),
            preferred_element_type=F32,
        )
        scores[g % 2, pl.ds(at, size), :] = s
        return jnp.maximum(top, jnp.max(s.reshape(size // 8, 8, wide_lanes), axis=0))

    def weigh(g, at, safe):
        size = min(CHUNK, n_keys - at)
        w = jnp.exp2((scores[g % 2, pl.ds(at, size), :] - safe) * SCALE)
        weights[g % 2, pl.ds(at, size), :] = w.astype(BF16)

    def finish(g, top):
        sums = jnp.dot(values_t[...], weights[g % 2], preferred_element_type=F32)
        mixed = sums[:HD].astype(BF16)
        total = sums[HD : HD + 1]
        t0 = total.astype(BF16)
        t1 = (total - t0.astype(F32)).astype(BF16)
        m0 = top.astype(BF16)
        rest = top - m0.astype(F32)
        m1 = rest.astype(BF16)
        m2 = (rest - m1.astype(F32)).astype(BF16)
        zero = jnp.zeros((STAT - 5, wide_lanes), BF16)
        stat = jnp.concatenate([m0, m1, m2, t0, t1, zero], axis=0)
        for i in range(PEERS):
            out[g * PEERS + i, pl.ds(0, HD), :] = mixed[:, i * lanes : (i + 1) * lanes]
            out[g * PEERS + i, pl.ds(HD, STAT), :] = stat[:, i * lanes : (i + 1) * lanes]

    tops = {}
    for step in range(groups + 2):
        now, last, done = step, step - 1, step - 2
        if now < groups:
            set_queries(now)
            top = jnp.full((8, wide_lanes), -4.0 * BIG, F32)
        if 0 <= last < groups:
            safe = jnp.maximum(tops[last], FLOOR)
        for at in starts:
            if now < groups:
                top = score(now, at, top)
            if 0 <= last < groups:
                weigh(last, at, safe)
        if 0 <= done:
            finish(done, tops[done])
        if now < groups:
            tops[now] = jnp.max(top, axis=0, keepdims=True)


def combine_kernel(parts, weight, rows, given):
    heads = rows.shape[1] // HD
    peers = parts.shape[0]
    tops, totals = [], []
    for p in range(peers):
        stat = parts[p, pl.ds(HD, STAT), :].astype(F32)
        tops.append(stat[0:1] + stat[1:2] + stat[2:3])
        totals.append(stat[3:4] + stat[4:5])
    top = tops[0]
    for p in range(1, peers):
        top = jnp.maximum(top, tops[p])
    total = jnp.zeros_like(top)
    factors = []
    for p in range(peers):
        factor = jnp.exp2((tops[p] - top) * SCALE)
        total = total + factor * totals[p]
        factors.append(factor)
    total = 1.0 / total
    factors = [f * total for f in factors]
    mixed = parts[0, pl.ds(0, HD), :].astype(F32) * factors[0]
    for p in range(1, peers):
        mixed = mixed + parts[p, pl.ds(0, HD), :].astype(F32) * factors[p]
    turned = mixed.T.astype(BF16)
    for b in range(2):
        for h in range(heads):
            at = (b * heads + h) * BLOCK
            rows[pl.ds(b * BLOCK, BLOCK), pl.ds(h * HD, HD)] = turned[at : at + BLOCK]
    project(rows, weight, given, 1 - lax.axis_index("c"))


def keep_kernel(rows, weight, kept):
    project(rows, weight, kept, lax.axis_index("c"))


def project(rows, weight, out, core):
    step = out.shape[2]
    for x in range(out.shape[0]):
        columns = pl.ds(pl.multiple_of((2 * x + core) * step, step), step)
        out[x] = jnp.dot(rows[...], weight[:, columns], preferred_element_type=F32).astype(out.dtype)


def body(queries, keys, values, out_weight, doc_lengths, stretch_place):
    tok, q_width = queries.shape
    heads = q_width // HD
    ny, nz, nx = lax.axis_size("y"), lax.axis_size("z"), lax.axis_size("x")
    lanes = 2 * heads * BLOCK
    table = rope_tables(stretch_place.shape[0])
    vmem = pl.BlockSpec(memory_space=pltpu.VMEM)
    hbm = pl.BlockSpec(memory_space=pltpu.HBM)
    n_place = stretch_place.shape[0]
    n_docs = doc_lengths.shape[0]
    q_rot, kv = pl.pallas_call(
        rotate_kernel,
        out_shape=(jax.ShapeDtypeStruct((ny, tok, q_width), BF16), jax.ShapeDtypeStruct((tok, 2 * HD), BF16)),
        in_specs=[hbm] * 5,
        out_specs=(vmem, vmem),
        scratch_shapes=[
            pltpu.SMEM((n_place,), jnp.int32),
            pltpu.VMEM((tok, q_width), BF16),
            pltpu.VMEM((tok, HD), BF16),
            pltpu.VMEM((tok, HD), BF16),
            pltpu.VMEM(table.shape, F32),
            pltpu.SemaphoreType.DMA((5,)),
        ],
        compiler_params=pltpu.CompilerParams(vmem_limit_bytes=4 << 20),
        name="rotate",
    )(*[pltpu.with_memory_space_constraint(a, pltpu.HBM) for a in (stretch_place, queries, keys, values, jnp.asarray(table))])
    q_all = lax.all_to_all(q_rot, "y", split_axis=0, concat_axis=0, tiled=True)
    kv_all = lax.all_gather(kv, "z", axis=0, tiled=True)
    n_keys = nz * tok
    pairs = ny * lanes * n_keys
    parts = pl.pallas_call(
        attend_kernel,
        out_shape=jax.ShapeDtypeStruct((ny, HD + STAT, lanes), BF16),
        in_specs=[hbm, hbm, vmem, vmem],
        out_specs=vmem,
        scratch_shapes=[
            pltpu.SMEM((n_place,), jnp.int32),
            pltpu.SMEM((n_docs,), jnp.int32),
            pltpu.VMEM((2, n_keys, PEERS * lanes), F32),
            pltpu.VMEM((2, n_keys, PEERS * lanes), BF16),
            pltpu.VMEM((HD + STAT, n_keys), BF16),
            pltpu.VMEM((n_keys, 2 * HD), BF16),
            pltpu.VMEM((2, PEERS * lanes, 2 * HD), BF16),
            pltpu.SemaphoreType.DMA((2,)),
        ],
        compiler_params=pltpu.CompilerParams(vmem_limit_bytes=28 << 20),
        cost_estimate=pl.CostEstimate(flops=4 * pairs * HD, bytes_accessed=4 << 20, transcendentals=pairs),
        name="attend",
    )(
        pltpu.with_memory_space_constraint(stretch_place, pltpu.HBM),
        pltpu.with_memory_space_constraint(doc_lengths, pltpu.HBM),
        q_all,
        kv_all,
    )
    parts = lax.all_to_all(parts, "y", split_axis=0, concat_axis=0, tiled=True)
    step = out_weight.shape[1] // (2 * nx)
    half_flops = 2 * tok * q_width * nx * step
    cost = pl.CostEstimate(flops=half_flops, bytes_accessed=4 << 20, transcendentals=0)
    rows, given = pl.pallas_call(
        combine_kernel,
        out_shape=(jax.ShapeDtypeStruct((tok, q_width), BF16), jax.ShapeDtypeStruct((nx, tok, step), BF16)),
        in_specs=[vmem, vmem],
        out_specs=(vmem, vmem),
        compiler_params=pltpu.CompilerParams(vmem_limit_bytes=8 << 20),
        cost_estimate=cost,
        name="combine",
    )(parts, out_weight)
    got = lax.ppermute(given, "c", [(0, 1), (1, 0)])
    kept = pl.pallas_call(
        keep_kernel,
        out_shape=jax.ShapeDtypeStruct((nx, tok, step), F32),
        in_specs=[vmem, vmem],
        out_specs=vmem,
        compiler_params=pltpu.CompilerParams(vmem_limit_bytes=8 << 20),
        cost_estimate=cost,
        name="keep",
    )(rows, out_weight)
    both = (kept + got.astype(F32)).astype(BF16)
    arrived = lax.all_to_all(both, "x", split_axis=0, concat_axis=0, tiled=True)
    return arrived.astype(F32).sum(axis=0).astype(BF16)


def solution(mesh, ny=8):
    n_seq, n_tensor = mesh.devices.shape
    shape = (ny, n_seq // ny, n_tensor // 2, 2)
    inner = Mesh(mesh.devices.reshape(shape), ("y", "z", "x", "c"))
    seq, tensor = ("y", "z"), ("x", "c")
    split = P(seq, tensor)
    in_specs = (split, split, split, P(tensor, None), P(), P())
    return jax.shard_map(body, mesh=inner, in_specs=in_specs, out_specs=split, check_vma=False)
```

```python
import math

import jax
import jax.numpy as jnp
import numpy as np
from jax import lax
from jax.experimental import pallas as pl
from jax.experimental.pallas import tpu as pltpu
from jax.sharding import Mesh
from jax.sharding import PartitionSpec as P

HD = 128
HALF = HD // 2
BLOCK = 48
ROPE_BASE = 500000.0
BIG = 2.0**100
FLOOR = -1e29
FAR = 1 << 30
STAT = 8
CHUNK = 384
PEERS = 2
SCALE = math.log2(math.e) / math.sqrt(HD)
BF16 = jnp.bfloat16
F32 = jnp.float32


def rope_tables(blocks):
    freqs = ROPE_BASE ** (-(2.0 / HD) * np.arange(HALF, dtype=np.float64))
    freqs = np.concatenate([freqs, freqs])
    start = (BLOCK * np.arange(blocks, dtype=np.float64))[:, None] * freqs
    row = np.arange(BLOCK, dtype=np.float64)[:, None] * freqs
    return np.concatenate([np.cos(row), np.sin(row), np.cos(start), np.sin(start)]).astype(np.float32)


def rotate_kernel(
    place_in, docs_in, q_in, k_in, v_in, table_in,
    q_out, kv_out, place_out, docs_out,
    place, q, k, v, table, turned, sems, out_sems,
):
    sources = (place_in, table_in, q_in, k_in, v_in, place_in, docs_in)
    targets = (place, table, q, k, v, place_out, docs_out)
    copies = [pltpu.make_async_copy(s, d, sems.at[i]) for i, (s, d) in enumerate(zip(sources, targets))]
    for copy in copies:
        copy.start()
    for copy in copies[:3]:
        copy.wait()
    heads = q.shape[1] // HD
    blocks = place.shape[0]
    first = lax.axis_index("y") * lax.axis_size("z") + lax.axis_index("z")
    lane = lax.broadcasted_iota(jnp.int32, (BLOCK, HD), 1)
    cos_row = table[pl.ds(0, BLOCK), :]
    sin_row = table[pl.ds(BLOCK, BLOCK), :]
    factors = []
    for b in range(2):
        at = place[first * 2 + b]
        c0 = table[pl.ds(2 * BLOCK + at, 1), :]
        s0 = table[pl.ds(2 * BLOCK + blocks + at, 1), :]
        cosine = c0 * cos_row - s0 * sin_row
        sine = s0 * cos_row + c0 * sin_row
        factors.append((cosine, jnp.where(lane < HALF, -sine, sine)))
    for b in range(2):
        cosine, sine = factors[b]
        rows = pl.ds(b * BLOCK, BLOCK)
        for h in range(heads):
            x = q[rows, pl.ds(h * HD, HD)].astype(F32)
            turned[rows, pl.ds(h * HD, HD)] = (x * cosine + pltpu.roll(x, HALF, 1) * sine).astype(BF16)
    sends = [pltpu.make_async_copy(turned, q_out.at[p], out_sems.at[p]) for p in range(q_out.shape[0])]
    for send in sends:
        send.start()
    for copy in copies[3:]:
        copy.wait()
    for b in range(2):
        cosine, sine = factors[b]
        rows = pl.ds(b * BLOCK, BLOCK)
        x = k[rows, :].astype(F32)
        kv_out[rows, pl.ds(0, HD)] = (x * cosine + pltpu.roll(x, HALF, 1) * sine).astype(BF16)
        kv_out[rows, pl.ds(HD, HD)] = v[rows, :]
    for send in sends:
        send.wait()


def attend_kernel(place_in, docs_in, q, kv, out, place, docs, scores, weights, values_t, keys, queries, sems):
    copies = [
        pltpu.make_async_copy(place_in, place, sems.at[0]),
        pltpu.make_async_copy(docs_in, docs, sems.at[1]),
    ]
    for copy in copies:
        copy.start()
    peers, tok, width = q.shape
    heads = width // HD
    lanes = 2 * heads * BLOCK
    n_keys = kv.shape[0]
    n_blocks = n_keys // BLOCK
    n_docs = docs.shape[0]
    z_size = lax.axis_size("z")
    my_y = lax.axis_index("y")
    my_z = lax.axis_index("z")
    keys[:, pl.ds(0, HD)] = kv[:, pl.ds(0, HD)]
    for copy in copies:
        copy.wait()

    lane = lax.broadcasted_iota(jnp.int32, (1, HD), 1)
    begin = jnp.full((1, HD), FAR, jnp.int32)
    end = jnp.full((1, HD), FAR, jnp.int32)
    edge = jnp.int32(0)
    for d in range(n_docs):
        begin = jnp.where(lane == d, edge, begin)
        edge = edge + docs[d]
        end = jnp.where(lane == d, edge, end)
    causal_at = n_docs
    own_at = causal_at + 2 * peers
    assert own_at + 2 * BLOCK <= HD
    for p in range(peers):
        for b in range(2):
            after = (place[(p * z_size + my_z) * 2 + b] + 1) * BLOCK
            begin = jnp.where(lane == causal_at + 2 * p + b, after, begin)
    for b in range(2):
        at = own_at + b * BLOCK
        mine = (lane >= at) & (lane < at + BLOCK)
        key_at = place[(my_y * z_size + my_z) * 2 + b] * BLOCK + lane - at
        begin = jnp.where(mine, key_at, begin)
        end = jnp.where(mine, key_at + 1, end)

    row = lax.broadcasted_iota(jnp.int32, (BLOCK, HD), 0)
    wide = lax.broadcasted_iota(jnp.int32, (BLOCK, HD), 1)

    def key_columns(first, last):
        for j in range(first, last):
            k_pos = row + place[my_y * n_blocks + j] * BLOCK
            inside = (k_pos >= begin) & (k_pos < end)
            keys[pl.ds(j * BLOCK, BLOCK), pl.ds(HD, HD)] = jnp.where(inside, -BIG, 0.0).astype(BF16)

    groups = peers // PEERS
    wide_lanes = PEERS * lanes
    starts = list(range(0, n_keys, CHUNK))

    def set_queries(g):
        for i in range(PEERS):
            p = g * PEERS + i
            for b in range(2):
                q_pos = row + place[(p * z_size + my_z) * 2 + b] * BLOCK
                doc = jnp.where((q_pos < begin) | (q_pos >= end), 1.0, 0.0)
                block = jnp.where((q_pos >= begin - BLOCK) & (q_pos < begin), 1.0, 0.0)
                later = jnp.where(q_pos < begin, 1.0, 0.0)
                columns = jnp.where(wide < causal_at, doc, jnp.where(wide < own_at, block, later)).astype(BF16)
                for h in range(heads):
                    rows = pl.ds(((i * 2 + b) * heads + h) * BLOCK, BLOCK)
                    queries[g % 2, rows, pl.ds(0, HD)] = q[p, pl.ds(b * BLOCK, BLOCK), pl.ds(h * HD, HD)]
                    queries[g % 2, rows, pl.ds(HD, HD)] = columns

    def score(g, at, top):
        size = min(CHUNK, n_keys - at)
        s = lax.dot_general(
            keys[pl.ds(at, size), :],
            queries[g % 2],
            (((1,), (1,)), ((), ())),
            preferred_element_type=F32,
        )
        scores[g % 2, pl.ds(at, size), :] = s
        return jnp.maximum(top, jnp.max(s.reshape(size // 8, 8, wide_lanes), axis=0))

    def weigh(g, at, safe):
        size = min(CHUNK, n_keys - at)
        w = jnp.exp2((scores[g % 2, pl.ds(at, size), :] - safe) * SCALE)
        weights[g % 2, pl.ds(at, size), :] = w.astype(BF16)

    def finish(g, top):
        sums = jnp.dot(values_t[...], weights[g % 2], preferred_element_type=F32)
        mixed = sums[:HD].astype(BF16)
        total = sums[HD : HD + 1]
        t0 = total.astype(BF16)
        t1 = (total - t0.astype(F32)).astype(BF16)
        m0 = top.astype(BF16)
        rest = top - m0.astype(F32)
        m1 = rest.astype(BF16)
        m2 = (rest - m1.astype(F32)).astype(BF16)
        zero = jnp.zeros((STAT - 5, wide_lanes), BF16)
        stat = jnp.concatenate([m0, m1, m2, t0, t1, zero], axis=0)
        for i in range(PEERS):
            out[g * PEERS + i, pl.ds(0, HD), :] = mixed[:, i * lanes : (i + 1) * lanes]
            out[g * PEERS + i, pl.ds(HD, STAT), :] = stat[:, i * lanes : (i + 1) * lanes]

    tops = {}
    for step in range(groups + 2):
        now, last, done = step, step - 1, step - 2
        if now < groups:
            set_queries(now)
            top = jnp.full((8, wide_lanes), -4.0 * BIG, F32)
        if 0 <= last < groups:
            safe = jnp.maximum(tops[last], FLOOR)
        for at in starts:
            if now == 0:
                key_columns(at // BLOCK, min(at + CHUNK, n_keys) // BLOCK)
            if now < groups:
                top = score(now, at, top)
            if 0 <= last < groups:
                weigh(last, at, safe)
        if now == 0:
            values_t[pl.ds(0, HD), :] = kv[:, pl.ds(HD, HD)].T
            values_t[pl.ds(HD, STAT), :] = jnp.ones((STAT, n_keys), BF16)
        if 0 <= done:
            finish(done, tops[done])
        if now < groups:
            tops[now] = jnp.max(top, axis=0, keepdims=True)


def combine_kernel(parts, weight, rows, given):
    heads = rows.shape[1] // HD
    peers = parts.shape[0]
    tops, totals = [], []
    for p in range(peers):
        stat = parts[p, pl.ds(HD, STAT), :].astype(F32)
        tops.append(stat[0:1] + stat[1:2] + stat[2:3])
        totals.append(stat[3:4] + stat[4:5])
    top = tops[0]
    for p in range(1, peers):
        top = jnp.maximum(top, tops[p])
    total = jnp.zeros_like(top)
    factors = []
    for p in range(peers):
        factor = jnp.exp2((tops[p] - top) * SCALE)
        total = total + factor * totals[p]
        factors.append(factor)
    total = 1.0 / total
    factors = [f * total for f in factors]
    mixed = parts[0, pl.ds(0, HD), :].astype(F32) * factors[0]
    for p in range(1, peers):
        mixed = mixed + parts[p, pl.ds(0, HD), :].astype(F32) * factors[p]
    turned = mixed.T.astype(BF16)
    for b in range(2):
        for h in range(heads):
            at = (b * heads + h) * BLOCK
            rows[pl.ds(b * BLOCK, BLOCK), pl.ds(h * HD, HD)] = turned[at : at + BLOCK]
    project(rows, weight, given, 1 - lax.axis_index("c"))


def keep_kernel(rows, weight, kept):
    project(rows, weight, kept, lax.axis_index("c"))


def project(rows, weight, out, core):
    step = out.shape[2]
    for x in range(out.shape[0]):
        columns = pl.ds(pl.multiple_of((2 * x + core) * step, step), step)
        out[x] = jnp.dot(rows[...], weight[:, columns], preferred_element_type=F32).astype(out.dtype)


def body(queries, keys, values, out_weight, doc_lengths, stretch_place):
    tok, q_width = queries.shape
    heads = q_width // HD
    ny, nz, nx = lax.axis_size("y"), lax.axis_size("z"), lax.axis_size("x")
    lanes = 2 * heads * BLOCK
    table = rope_tables(stretch_place.shape[0])
    vmem = pl.BlockSpec(memory_space=pltpu.VMEM)
    hbm = pl.BlockSpec(memory_space=pltpu.HBM)
    n_place = stretch_place.shape[0]
    n_docs = doc_lengths.shape[0]
    n_inputs = 6
    args = (stretch_place, doc_lengths, queries, keys, values, jnp.asarray(table))
    q_rot, kv, place, docs = pl.pallas_call(
        rotate_kernel,
        out_shape=(
            jax.ShapeDtypeStruct((ny, tok, q_width), BF16),
            jax.ShapeDtypeStruct((tok, 2 * HD), BF16),
            jax.ShapeDtypeStruct((n_place,), jnp.int32),
            jax.ShapeDtypeStruct((n_docs,), jnp.int32),
        ),
        in_specs=[hbm] * n_inputs,
        out_specs=(hbm, vmem, vmem, vmem),
        scratch_shapes=[
            pltpu.SMEM((n_place,), jnp.int32),
            pltpu.VMEM((tok, q_width), BF16),
            pltpu.VMEM((tok, HD), BF16),
            pltpu.VMEM((tok, HD), BF16),
            pltpu.VMEM(table.shape, F32),
            pltpu.VMEM((tok, q_width), BF16),
            pltpu.SemaphoreType.DMA((n_inputs + 1,)),
            pltpu.SemaphoreType.DMA((ny,)),
        ],
        compiler_params=pltpu.CompilerParams(vmem_limit_bytes=4 << 20),
        name="rotate",
    )(*[pltpu.with_memory_space_constraint(a, pltpu.HBM) for a in args])
    q_all = lax.all_to_all(q_rot, "y", split_axis=0, concat_axis=0, tiled=True)
    kv_all = lax.all_gather(kv, "z", axis=0, tiled=True)
    n_keys = nz * tok
    pairs = ny * lanes * n_keys
    parts = pl.pallas_call(
        attend_kernel,
        out_shape=jax.ShapeDtypeStruct((ny, HD + STAT, lanes), BF16),
        in_specs=[vmem, vmem, vmem, vmem],
        out_specs=vmem,
        scratch_shapes=[
            pltpu.SMEM((n_place,), jnp.int32),
            pltpu.SMEM((n_docs,), jnp.int32),
            pltpu.VMEM((2, n_keys, PEERS * lanes), F32),
            pltpu.VMEM((2, n_keys, PEERS * lanes), BF16),
            pltpu.VMEM((HD + STAT, n_keys), BF16),
            pltpu.VMEM((n_keys, 2 * HD), BF16),
            pltpu.VMEM((2, PEERS * lanes, 2 * HD), BF16),
            pltpu.SemaphoreType.DMA((2,)),
        ],
        compiler_params=pltpu.CompilerParams(vmem_limit_bytes=28 << 20),
        cost_estimate=pl.CostEstimate(flops=4 * pairs * HD, bytes_accessed=4 << 20, transcendentals=pairs),
        name="attend",
    )(
        place,
        docs,
        q_all,
        kv_all,
    )
    parts = lax.all_to_all(parts, "y", split_axis=0, concat_axis=0, tiled=True)
    step = out_weight.shape[1] // (2 * nx)
    half_flops = 2 * tok * q_width * nx * step
    cost = pl.CostEstimate(flops=half_flops, bytes_accessed=4 << 20, transcendentals=0)
    rows, given = pl.pallas_call(
        combine_kernel,
        out_shape=(jax.ShapeDtypeStruct((tok, q_width), BF16), jax.ShapeDtypeStruct((nx, tok, step), BF16)),
        in_specs=[vmem, vmem],
        out_specs=(vmem, vmem),
        compiler_params=pltpu.CompilerParams(vmem_limit_bytes=8 << 20),
        cost_estimate=cost,
        name="combine",
    )(parts, out_weight)
    got = lax.ppermute(given, "c", [(0, 1), (1, 0)])
    kept = pl.pallas_call(
        keep_kernel,
        out_shape=jax.ShapeDtypeStruct((nx, tok, step), F32),
        in_specs=[vmem, vmem],
        out_specs=vmem,
        compiler_params=pltpu.CompilerParams(vmem_limit_bytes=8 << 20),
        cost_estimate=cost,
        name="keep",
    )(rows, out_weight)
    both = (kept + got.astype(F32)).astype(BF16)
    arrived = lax.all_to_all(both, "x", split_axis=0, concat_axis=0, tiled=True)
    return arrived.astype(F32).sum(axis=0).astype(BF16)


def solution(mesh, ny=8):
    n_seq, n_tensor = mesh.devices.shape
    shape = (ny, n_seq // ny, n_tensor // 2, 2)
    inner = Mesh(mesh.devices.reshape(shape), ("y", "z", "x", "c"))
    seq, tensor = ("y", "z"), ("x", "c")
    split = P(seq, tensor)
    in_specs = (split, split, split, P(tensor, None), P(), P())
    return jax.shard_map(body, mesh=inner, in_specs=in_specs, out_specs=split, check_vma=False)
```
